32 devices in a mesh: dp: 2 (over x), expert: 16 (over z, y, core).
Axes of the slice: x: 2, y: 2, z: 4, core: 2. Of those that a mesh axis runs over, the one named last changes fastest.
Arguments:
- hidden: bfloat16 [2, 1024, 2, 2048], P('dp', 'expert'), may hold values from -6 to 6
- queries: bfloat16 [2, 1024, 2, 4096], P('dp', 'expert'), may hold values from -45 to 45
- latents: bfloat16 [2, 1024, 2, 512], P('dp', 'expert'), may hold values from -165 to 165
- mem_latents: bfloat16 [2, 32, 2, 512], P('dp'), may hold values from -6 to 6
- lengths: int32 [2, 2], P('dp'), may hold values from 512 to 1024
- ids: int32 [2, 1024, 2, 6], P('dp', 'expert'), may hold values from 0 to 15, all different within a row; in each aligned block of 128 rows (0 to 127, 128 to 255, ..., all dimensions but the last counted through in order) at most 50 rows name the same one
- gates: bfloat16 [2, 1024, 2, 6], P('dp', 'expert'), may hold values from 0.049804688 to 0.5
- norm_gain: bfloat16 [2048], replicated, may hold values from 0.25 to 1.75
- w_uv: bfloat16 [8, 512, 128], P('dp'), may hold values from -0.25 to 0.25
- w_out: bfloat16 [1024, 2048], P('dp'), may hold values from -0.1875 to 0.1875
- w_gate: bfloat16 [16, 2048, 704], P('expert'), may hold values from -0.125 to 0.125
- w_up: bfloat16 [16, 2048, 704], P('expert'), may hold values from -0.125 to 0.125
- w_down: bfloat16 [16, 704, 2048], P('expert'), may hold values from -0.21875 to 0.21875
Outputs:
- layer_out: bfloat16 [2, 1024, 2, 2048], P('dp', 'expert')
The draws below stay inside these ranges and needn't reach their ends.
Inputs may be any that keep to these rules, and one draw needn't show every extreme that they name: `ids`: each row names 6 different experts; the rows of one device (aligned blocks of 128 rows in the order of the leading dimensions) name any one expert at most 50 times, a bound that some block reaches.
All inputs are finite; a program needn't handle non-finite values.
Results may differ from the reference program's by a relative error of at most 0.007.
Values may be sent and summed in bfloat16 or wider, within the bound.
A program may use at most 128 MiB of HBM per device.

```python
import math
import jax
import jax.numpy as jnp
import numpy as np
from jax import lax

D = 2048
HEADS = 8
LAT = 512
VDIM = 128
FF = 704
TOPK = 6
MEM = 32
SEQS = 2
SEG = 1024
TOK_DEV = 128
EXPERTS = 16
CAP = 50
N_DP = 2
N_EXPERT = 16


def draw_latents(key, part):
    entries = jnp.clip(jax.random.normal(jax.random.fold_in(key, 1), (N_DP, SEG, SEQS, LAT), jnp.float32), -6.0, 6.0)
    return entries.astype(jnp.bfloat16)


def draw_queries(key, part):
    full_shape = (N_DP, SEG, SEQS, HEADS, LAT)
    entries = 0.5 * jnp.clip(jax.random.normal(jax.random.fold_in(key, 3), full_shape, jnp.float32), -6.0, 6.0)
    return entries.reshape(N_DP, SEG, SEQS, HEADS * LAT).astype(jnp.bfloat16)


def set_ends(drawn, rng, low, largest):
    spot = [jax.random.randint(jax.random.fold_in(rng, axis), (), 0, length) for axis, length in enumerate(drawn.shape)]
    longest = drawn.shape.index(max(drawn.shape))
    neighbour = spot[:longest] + [(spot[longest] + 1) % drawn.shape[longest]] + spot[longest + 1:]
    return drawn.at[tuple(spot)].set(low).at[tuple(neighbour)].set(largest)


def steps_of(key, extent, shards, least, high):
    level, own = 1.0, jax.random.fold_in(key, 6)
    for dim, parts in shards:
        heights = jnp.exp(jax.random.uniform(jax.random.fold_in(own, dim), (parts,), jnp.float32, least / len(shards), high / len(shards)))
        level = level * jnp.repeat(heights, extent[dim] // parts).reshape([-1 if axis == dim else 1 for axis in range(len(extent))])
    return level


def routed_block(own_key, own, number, rows, number_of, top, most, slope):
    ranking = jax.random.permutation(own_key, number_of)
    crowded, ordinary = portions_of(number_of, rows * top, most, slope, True), portions_of(number_of, rows * top, most, slope, False)
    places = jnp.arange(number_of)

    def named(sizes, offset_by):
        used = int((sizes > 0).sum())
        fixed = max(1, used // 4)
        moved = fixed + (places - fixed + offset_by * (used - fixed)) % max(1, number_of - fixed)
        return jnp.zeros((number_of,), jnp.int32).at[ranking[jnp.where(places < fixed, places, moved)]].set(jnp.asarray(sizes, jnp.int32))

    sizes = jnp.where(number % 4 == 0, named(crowded, number // 4), named(ordinary, number - number // 4 - 1))
    mixed = jax.random.permutation(jax.random.fold_in(own, 3), number_of)
    giver, sink = mixed[0:number_of // 2 * 2:2], mixed[1:number_of // 2 * 2:2]
    margin = jnp.minimum(sizes[giver] - 1, most - sizes[sink]) // 2
    margin = jnp.where((giver == ranking[0]) | (sink == ranking[0]) | (sizes[sink] == 0), 0, jnp.maximum(margin, 0))
    moved = jax.random.randint(jax.random.fold_in(own, 4), (number_of // 2,), 0, 1 << 20) % (margin + 1)
    sizes = sizes.at[giver].add(-moved).at[sink].add(moved)
    labels = jnp.searchsorted(jnp.cumsum(sizes), jnp.arange(rows * top), side="right").astype(jnp.int32)
    table = labels.reshape(top, rows).T
    table = table[jax.random.permutation(jax.random.fold_in(own, 1), rows)]
    offset_by = jax.random.randint(jax.random.fold_in(own, 2), (rows, 1), 0, top)
    return jnp.take_along_axis(table, (jnp.arange(top)[None, :] + offset_by) % top, axis=1)


def portions_of(number_of, total, reach, skew, full):
    weights = [(1 << 20) // math.isqrt(grade ** skew) + 1 for grade in range(1, number_of + 1)]
    largest = reach if full else min(reach, max(-(-total // number_of), total * weights[0] // sum(weights)))
    least = 1 if total - largest >= number_of - 1 else 0
    given, surplus = [largest] + [least] * (number_of - 1), total - largest - least * (number_of - 1)
    while surplus > 0:
        candidates = [i for i in range(1, number_of) if given[i] < largest] or [i for i in range(1, number_of) if given[i] < reach]
        pool, budget = sum([weights[i] for i in candidates]), surplus
        for i in candidates:
            extra = min(reach - given[i], max(1, budget * weights[i] // pool), surplus)
            given[i] = given[i] + extra
            surplus = surplus - extra
    return np.array(given)


def scatter_about(key, shape, scale, most, cuts=(), held_as=jnp.bfloat16):
    values = jax.random.normal(key, shape, jnp.float32) * scale
    if len(cuts) > 0:
        values = steps_of(key, shape, cuts, -0.22, 0.18) * values
    return jnp.clip(values, min=-most, max=most).astype(held_as)


def setup_inputs(seed: int = 0) -> dict:
    arg_keys = jax.random.split(jax.random.key(seed), 14)
    hidden = scatter_about(arg_keys[0], (N_DP, SEG, SEQS, D), 1.0, 6.0, ((0, 2), (1, 16)))
    queries = draw_queries(jax.random.fold_in(arg_keys[13], 71), 0)
    latents = draw_latents(jax.random.fold_in(arg_keys[13], 71), 0)
    mem_latents = scatter_about(arg_keys[3], (N_DP, MEM, SEQS, LAT), 1.0, 6.0, ((0, 2),))
    lengths = set_ends(jax.random.randint(arg_keys[4], (N_DP, SEQS), SEG // 2, SEG + 1), jax.random.fold_in(arg_keys[4], 1), SEG // 2, SEG).astype(jnp.int32)
    ids_keys = jax.random.split(jax.random.fold_in(arg_keys[5], 1), N_DP * SEG * SEQS // TOK_DEV)
    ids_turns = jax.random.permutation(jax.random.fold_in(arg_keys[5], 3), N_DP * SEG * SEQS // TOK_DEV)
    ids = jax.vmap(lambda own, number: routed_block(jax.random.fold_in(arg_keys[5], 2), own, number, TOK_DEV, EXPERTS, TOPK, CAP, 2))(ids_keys, ids_turns).reshape((N_DP, SEG, SEQS, TOPK))
    gates = jnp.clip(jnp.exp(math.log(0.5) - 2.306499 * jax.random.uniform(arg_keys[6], (N_DP, SEG, SEQS, TOPK), jnp.float32) ** steps_of(arg_keys[6], (N_DP, SEG, SEQS, TOPK), ((0, 2), (1, 16)), -0.2, 0.2)), 0.049804688, 0.5).astype(jnp.bfloat16)
    norm_gain = jnp.clip(1.0 + 0.15 * jax.random.normal(arg_keys[7], (D,), jnp.float32), 0.25, 1.75).astype(jnp.bfloat16)
    w_uv = scatter_about(arg_keys[8], (HEADS, LAT, VDIM), LAT ** -0.5, 0.25, ((0, 2),))
    w_out = scatter_about(arg_keys[9], (HEADS * VDIM, D), (HEADS * VDIM) ** -0.5, 0.1875, ((0, 2),))
    w_gate = scatter_about(arg_keys[10], (EXPERTS, D, FF), D ** -0.5, 0.125, ((0, 16),))
    w_up = scatter_about(arg_keys[11], (EXPERTS, D, FF), D ** -0.5, 0.125, ((0, 16),))
    w_down = scatter_about(arg_keys[12], (EXPERTS, FF, D), FF ** -0.5, 0.21875, ((0, 16),))
    return {"hidden": hidden, "queries": queries, "latents": latents, "mem_latents": mem_latents, "lengths": lengths, "ids": ids, "gates": gates, "norm_gain": norm_gain, "w_uv": w_uv, "w_out": w_out, "w_gate": w_gate, "w_up": w_up, "w_down": w_down}


score_scale = 192.0 ** (-0.5)
norm_eps = 1e-06

def attend_one(query_rows, seg_latent, mem_latent, seq_limit):
    key_rows = jnp.concatenate([mem_latent, seg_latent], axis=0).astype(jnp.float32)
    scores = jnp.einsum('ihl,jl->hij', query_rows.astype(jnp.float32), key_rows) * score_scale
    query_pos = jnp.arange(SEG, dtype=jnp.int32)
    seg_visible = (query_pos[None, :] <= query_pos[:, None]) & (query_pos[None, :] < seq_limit)
    visible = jnp.concatenate([jnp.ones((SEG, MEM), dtype=bool), seg_visible], axis=1)
    scores = jnp.where(visible[None], scores, -jnp.inf)
    row_top = lax.optimization_barrier(jnp.max(scores, axis=2))
    weights = jnp.exp(scores - row_top[..., None])
    exp_total = lax.optimization_barrier(jnp.sum(weights, axis=2))
    rounded = lax.optimization_barrier(weights.astype(jnp.bfloat16)).astype(jnp.float32)
    attended = jnp.einsum('hij,jl->ihl', rounded, key_rows) / jnp.transpose(exp_total)[..., None]
    return attended.astype(jnp.bfloat16)

def reference(hidden, queries, latents, mem_latents, lengths, ids, gates, norm_gain, w_uv, w_out, w_gate, w_up, w_down):
    batch = N_DP * SEQS
    query_all = queries.reshape(N_DP, SEG, SEQS, HEADS, LAT).transpose(0, 2, 1, 3, 4).reshape(batch, SEG, HEADS, LAT)
    seg_all = latents.transpose(0, 2, 1, 3).reshape(batch, SEG, LAT)
    mem_all = mem_latents.transpose(0, 2, 1, 3).reshape(batch, MEM, LAT)
    limits = lengths.reshape(batch)
    attended = lax.map(lambda item: attend_one(item[0], item[1], item[2], item[3]), (query_all, seg_all, mem_all, limits))
    values = jnp.einsum('bihl,hlv->bihv', attended.astype(jnp.float32), w_uv.astype(jnp.float32)).astype(jnp.bfloat16)
    attn_out = jnp.dot(values.reshape(batch * SEG, HEADS * VDIM), w_out, preferred_element_type=jnp.float32)
    attn_out = attn_out.reshape(N_DP, SEQS, SEG, D).transpose(0, 2, 1, 3)
    residual = hidden.astype(jnp.float32) + attn_out
    mean_square = lax.optimization_barrier(jnp.mean(residual * residual, axis=-1, keepdims=True))
    normed = (residual * lax.rsqrt(mean_square + norm_eps) * norm_gain.astype(jnp.float32)).astype(jnp.bfloat16)
    row_total = N_DP * SEG * SEQS
    flat_normed = normed.reshape(row_total, D)
    flat_ids = ids.reshape(row_total * TOPK)
    flat_gates = gates.reshape(row_total * TOPK).astype(jnp.float32)
    reach_rows = N_DP * N_EXPERT * CAP

    def per_expert(running, item):
        gate_w, up_w, down_w, expert_id = item
        matches = flat_ids == expert_id
        picked = jnp.nonzero(matches, size=reach_rows, fill_value=0)[0].astype(jnp.int32)
        is_live = jnp.arange(reach_rows, dtype=jnp.int32) < jnp.sum(matches.astype(jnp.int32))
        token_index = (picked // TOPK).astype(jnp.int32)
        picked_rows = flat_normed[token_index]
        gate_h = jnp.dot(picked_rows, gate_w, preferred_element_type=jnp.float32)
        up_h = jnp.dot(picked_rows, up_w, preferred_element_type=jnp.float32)
        act = (jax.nn.silu(gate_h) * up_h).astype(jnp.bfloat16)
        out_rows = jnp.dot(act, down_w, preferred_element_type=jnp.float32).astype(jnp.bfloat16)
        out_rows = lax.optimization_barrier(out_rows).astype(jnp.float32)
        scale_w = jnp.where(is_live, flat_gates[picked], jnp.float32(0.0))
        running = running.at[token_index].add(scale_w[:, None] * out_rows)
        return (running, None)
    start_acc = jnp.zeros((row_total, D), jnp.float32)
    routed, unused = lax.scan(per_expert, start_acc, (w_gate, w_up, w_down, jnp.arange(EXPERTS, dtype=jnp.int32)))
    layer_out = residual + routed.reshape(N_DP, SEG, SEQS, D)
    return layer_out.astype(jnp.bfloat16)
```

```python
import functools

import jax
import jax.numpy as jnp
from jax import lax
from jax.experimental import pallas as pl
from jax.experimental.pallas import tpu as pltpu
from jax.sharding import PartitionSpec as P

score_scale = 192.0 ** (-0.5)
norm_eps = 1e-06
MESH = pl.DeviceIdType.MESH


def ring_place(n):
    chips = n // 2
    depth = chips // 2
    me = lax.axis_index("expert")
    core = me % 2
    chip = me // 2
    row, col = chip // 2, chip % 2
    pos = col * row + (1 - col) * (chips - 1 - row)

    def device(offset, core_of):
        p = (pos + offset + chips) % chips
        q = p // depth
        r = (1 - q) * p + q * (chips - 1 - p)
        return (2 * r + 1 - q) * 2 + core_of

    return me, core, device


def greet(targets):
    barrier = pltpu.get_barrier_semaphore()
    for target in targets:
        pl.semaphore_signal(barrier, inc=1, device_id={"expert": target}, device_id_type=MESH)
    pl.semaphore_wait(barrier, len(targets))


def remote(src, dst, send_sem, recv_sem, target):
    return pltpu.make_async_remote_copy(
        src_ref=src,
        dst_ref=dst,
        send_sem=send_sem,
        recv_sem=recv_sem,
        device_id={"expert": target},
        device_id_type=MESH,
    )


def gather_kernel(n, cut, x_ref, out_ref, ring_send, ring_recv, pair_send, pair_recv, own_sem):
    chips = n // 2
    half_ring = chips // 2
    rows = x_ref.shape[0]
    last = chips - 2
    me, core, device = ring_place(n)
    partner = device(0, 1 - core)
    ahead = (device(1, core), device(-1, core))
    spans = (pl.ds(0, cut), pl.ds(cut, rows - cut))
    greet((ahead[0], ahead[1], partner))

    def arrival(way, j):
        dist, half = (half_ring, way) if j == last else (j // 2 + 1, j % 2)
        return device(-dist if way == 0 else dist, core), spans[half]

    waits = []
    for way in (0, 1):
        for j in (0, 1):
            if j > last:
                continue
            if j == last and half_ring == 1:
                span = spans[way]
            else:
                span = spans[j]
            copy = remote(
                x_ref.at[span], out_ref.at[me, span],
                ring_send.at[way, j], ring_recv.at[way, j], ahead[way],
            )
            copy.start()
            waits.append(copy)
    share = remote(x_ref, out_ref.at[me], pair_send.at[2 * last + 2], pair_recv.at[2 * last + 2], partner)
    share.start()
    waits.append(share)
    keep = pltpu.make_async_copy(x_ref, out_ref.at[me], own_sem)
    keep.start()

    for j in range(last + 1):
        for way in (0, 1):
            slot, span = arrival(way, j)
            piece = out_ref.at[slot, span]
            remote(piece, piece, ring_send.at[way, j], ring_recv.at[way, j], ahead[way]).wait_recv()
            onward = j + 2
            if j >= last - 2 and j < last:
                onward = last if j == last - 2 + way else None
            if j == last:
                onward = None
            if onward is not None:
                copy = remote(piece, piece, ring_send.at[way, onward], ring_recv.at[way, onward], ahead[way])
                copy.start()
                waits.append(copy)
            index = 2 * j + way
            copy = remote(piece, piece, pair_send.at[index], pair_recv.at[index], partner)
            copy.start()
            waits.append(copy)

    for j in range(last + 1):
        for way in (0, 1):
            dist, half = (half_ring, way) if j == last else (j // 2 + 1, j % 2)
            slot = device(-dist if way == 0 else dist, 1 - core)
            piece = out_ref.at[slot, spans[half]]
            index = 2 * j + way
            remote(piece, piece, pair_send.at[index], pair_recv.at[index], partner).wait_recv()
    other = out_ref.at[partner]
    remote(other, other, pair_send.at[2 * last + 2], pair_recv.at[2 * last + 2], partner).wait_recv()
    for copy in waits:
        copy.wait_send()
    keep.wait()


def ring_gather(x, n, cut, collective_id):
    rows, cols = x.shape
    steps = n // 2 - 1
    return pl.pallas_call(
        functools.partial(gather_kernel, n, cut),
        out_shape=jax.ShapeDtypeStruct((n, rows, cols), x.dtype),
        in_specs=[pl.BlockSpec(memory_space=pltpu.VMEM)],
        out_specs=pl.BlockSpec(memory_space=pl.ANY),
        scratch_shapes=[
            pltpu.SemaphoreType.DMA((2, steps)),
            pltpu.SemaphoreType.DMA((2, steps)),
            pltpu.SemaphoreType.DMA((2 * steps + 1,)),
            pltpu.SemaphoreType.DMA((2 * steps + 1,)),
            pltpu.SemaphoreType.DMA,
        ],
        compiler_params=pltpu.CompilerParams(collective_id=collective_id, has_side_effects=True),
        cost_estimate=pl.CostEstimate(flops=0, bytes_accessed=16 * n * rows * cols, transcendentals=0),
        name="ring_gather_%d" % collective_id,
    )(x)


def reduce_kernel(
    n, part_ref, out_ref, mine, paired, arrived, ring_send, ring_recv, pair_send, pair_recv, load_sem
):
    chips = n // 2
    half_ring = chips // 2
    half = mine.shape[1] // 2
    last = chips - 2
    me, core, device = ring_place(n)
    partner = device(0, 1 - core)
    ahead = (device(1, core), device(-1, core))
    greet((ahead[0], ahead[1], partner))

    order = [half_ring]
    for k in range(half_ring - 1, 0, -1):
        order += [k, chips - k]
    order.append(0)
    loads, shares = {}, {}
    for k in order:
        shares[k] = remote(
            part_ref.at[device(k, 1 - core)], paired.at[k], pair_send.at[k], pair_recv.at[k], partner
        )
        shares[k].start()
        loads[k] = pltpu.make_async_copy(part_ref.at[device(k, core)], mine.at[k], load_sem.at[k])
        loads[k].start()

    ready = set()

    def bring(k):
        if k not in ready:
            ready.add(k)
            loads[k].wait()
            shares[k].wait_recv()

    def index_of(dist, h):
        return 0 if dist == half_ring else 1 + 2 * (half_ring - 1 - dist) + h

    def await_ring(way, j):
        piece = arrived.at[way, j]
        remote(piece, piece, ring_send.at[way, j], ring_recv.at[way, j], ahead[way]).wait_recv()

    sends = []
    for dist in range(half_ring, 0, -1):
        for turn in (0, 1):
            for way in (0, 1):
                if dist == half_ring:
                    if turn == 1:
                        continue
                    h = way
                elif dist == half_ring - 1:
                    h = 1 - way if turn == 0 else way
                else:
                    h = turn
                k = dist if way == 0 else chips - dist
                bring(k)
                span = pl.ds(h * half, half)
                total = mine[k, span].astype(jnp.float32) + paired[k, span].astype(jnp.float32)
                has_prior = dist < half_ring - 1 or (dist == half_ring - 1 and h == way)
                if has_prior:
                    j = index_of(dist + 1, h)
                    await_ring(way, j)
                    total = total + arrived[way, j].astype(jnp.float32)
                mine[k, span] = total.astype(mine.dtype)
                j = index_of(dist, h)
                copy = remote(
                    mine.at[k, span], arrived.at[way, j],
                    ring_send.at[way, j], ring_recv.at[way, j], ahead[way],
                )
                copy.start()
                sends.append(copy)
    bring(0)
    for h in (0, 1):
        span = pl.ds(h * half, half)
        total = mine[0, span].astype(jnp.float32) + paired[0, span].astype(jnp.float32)
        for way in (0, 1):
            j = index_of(1, h)
            await_ring(way, j)
            total = total + arrived[way, j].astype(jnp.float32)
        out_ref[span] = total
    for copy in sends:
        copy.wait_send()
    for k in order:
        shares[k].wait_send()


def ring_reduce(part, n, collective_id):
    rows, cols = part.shape[1:]
    chips = n // 2
    return pl.pallas_call(
        functools.partial(reduce_kernel, n),
        out_shape=jax.ShapeDtypeStruct((rows, cols), jnp.float32),
        in_specs=[pl.BlockSpec(memory_space=pl.ANY)],
        out_specs=pl.BlockSpec(memory_space=pltpu.VMEM),
        scratch_shapes=[
            pltpu.VMEM((chips, rows, cols), part.dtype),
            pltpu.VMEM((chips, rows, cols), part.dtype),
            pltpu.VMEM((2, chips - 1, rows // 2, cols), part.dtype),
            pltpu.SemaphoreType.DMA((2, chips - 1)),
            pltpu.SemaphoreType.DMA((2, chips - 1)),
            pltpu.SemaphoreType.DMA((chips,)),
            pltpu.SemaphoreType.DMA((chips,)),
            pltpu.SemaphoreType.DMA((chips,)),
        ],
        compiler_params=pltpu.CompilerParams(
            collective_id=collective_id, has_side_effects=True, vmem_limit_bytes=60 * 1024 * 1024
        ),
        cost_estimate=pl.CostEstimate(flops=0, bytes_accessed=16 * part.size, transcendentals=0),
        name="ring_reduce_%d" % collective_id,
    )(part)


def shards(
    hidden,
    queries,
    latents,
    mem_latents,
    lengths,
    ids,
    gates,
    norm_gain,
    w_uv,
    w_out,
    w_gate,
    w_up,
    w_down,
):
    f32, bf16 = jnp.float32, jnp.bfloat16
    local_len, seq_count, model_width = hidden.shape[1:]
    latent_dim = latents.shape[3]
    head_count = queries.shape[3] // latent_dim
    row_count = local_len * seq_count
    n = lax.axis_size("expert")
    dp_size = lax.axis_size("dp")
    me = lax.axis_index("expert")
    core = me % 2
    own_dp = lax.axis_index("dp")
    heads_here, _, value_dim = w_uv.shape
    top_count = ids.shape[3]

    half_heads = heads_here // 2
    uv_half = lax.dynamic_slice_in_dim(w_uv, core * half_heads, half_heads, 0)
    out_half = lax.dynamic_slice_in_dim(
        w_out, core * half_heads * value_dim, half_heads * value_dim, 0
    )
    uv_groups, out_groups, starts = [w_uv], [w_out], [own_dp * heads_here]
    swap = [(i, i ^ 1) for i in range(n)]
    sizes = [heads_here]
    for shift in range(1, dp_size):
        turn = [(i, (i + shift) % dp_size) for i in range(dp_size)]
        source = (own_dp - shift + dp_size) % dp_size
        uv_far = lax.ppermute(uv_half, "dp", turn)
        out_far = lax.ppermute(out_half, "dp", turn)
        uv_near = lax.ppermute(uv_far, "expert", swap)
        out_near = lax.ppermute(out_far, "expert", swap)
        uv_groups += [uv_far, uv_near]
        out_groups += [out_far, out_near]
        starts += [
            source * heads_here + core * half_heads,
            source * heads_here + (1 - core) * half_heads,
        ]
        sizes += [half_heads, half_heads]

    latent_rows = jnp.transpose(latents[0], (1, 0, 2)).reshape(row_count, latent_dim)
    ids_t = jnp.transpose(ids[0], (2, 1, 0)).reshape(top_count, row_count).astype(bf16)
    gates_t = jnp.transpose(gates[0], (2, 1, 0)).reshape(top_count, row_count)
    table = jnp.concatenate([ids_t, gates_t], axis=0).reshape(-1)
    table_rows = -(-table.shape[0] // (16 * latent_dim)) * 16
    table = jnp.pad(table, (0, table_rows * latent_dim - table.shape[0]))
    packed = jnp.concatenate([latent_rows, table.reshape(table_rows, latent_dim)], axis=0)
    all_rows = row_count + table_rows
    cut = (all_rows // 2 + 15) // 16 * 16
    gathered = ring_gather(packed, n, cut, 0)

    segment = gathered[:, :row_count].reshape(n, seq_count, local_len, latent_dim)
    segment = jnp.transpose(segment, (1, 0, 2, 3)).reshape(seq_count, n * local_len, latent_dim)
    memory = jnp.transpose(mem_latents[0], (1, 0, 2))
    mem_count = memory.shape[1]
    keys = jnp.concatenate([memory, segment], axis=1)
    query_rows = jnp.transpose(
        queries[0].reshape(local_len, seq_count, head_count, latent_dim), (1, 2, 0, 3)
    ).reshape(seq_count, head_count * local_len, latent_dim)
    scores = jnp.einsum("sql,sjl->sqj", query_rows, keys, preferred_element_type=f32) * score_scale
    key_pos = jnp.arange(keys.shape[1], dtype=jnp.int32) - mem_count
    own_pos = me * local_len + jnp.arange(local_len, dtype=jnp.int32)
    visible = (key_pos[None, None, :] <= own_pos[None, :, None]) & (
        key_pos[None, None, :] < lengths[0][:, None, None]
    )
    visible = visible | (key_pos < 0)[None, None, :]
    scores = scores.reshape(seq_count, head_count, local_len, -1)
    scores = jnp.where(visible[:, None], scores, -jnp.inf)
    weights = jnp.exp(scores - jnp.max(scores, axis=3, keepdims=True))
    total = jnp.sum(weights, axis=3)
    attended = jnp.einsum(
        "sqj,sjl->sql",
        weights.astype(bf16).reshape(seq_count, head_count * local_len, -1),
        keys,
        preferred_element_type=f32,
    ).reshape(seq_count, head_count, local_len, latent_dim)
    attended = (attended / total[..., None]).astype(bf16)

    attn_out = jnp.zeros((row_count, model_width), f32)
    for uv, out, start, size in zip(uv_groups, out_groups, starts, sizes):
        heads = lax.dynamic_slice_in_dim(attended, start, size, 1)
        values = jnp.einsum("shtl,hlv->sthv", heads, uv, preferred_element_type=f32).astype(bf16)
        attn_out = attn_out + jnp.dot(
            values.reshape(row_count, size * value_dim), out, preferred_element_type=f32
        )

    hidden_rows = jnp.transpose(hidden[0], (1, 0, 2)).reshape(row_count, model_width)
    residual = hidden_rows.astype(f32) + attn_out
    mean_square = jnp.mean(residual * residual, axis=-1, keepdims=True)
    normed = (residual * lax.rsqrt(mean_square + norm_eps) * norm_gain.astype(f32)).astype(bf16)

    rows_all = ring_gather(normed, n, row_count // 2, 1)
    experts_here = w_gate.shape[0]
    expert_count = n * experts_here
    capacity = min(row_count, row_count * top_count // expert_count + 2)
    groups = n // 2
    wide = 2 * row_count
    slots = -(-2 * capacity // 16) * 16
    tables = gathered[:, row_count:].reshape(n, -1)[:, : 2 * top_count * row_count]
    tables = tables.reshape(groups, 2, 2, top_count, row_count)
    named = jnp.transpose(tables[:, :, 0], (2, 0, 1, 3)).reshape(top_count, groups, wide)
    scale = jnp.transpose(tables[:, :, 1], (2, 0, 1, 3)).reshape(top_count, groups, wide)
    rows_all = rows_all.reshape(groups, wide, model_width)
    steps = jnp.arange(wide, dtype=jnp.int32)
    earlier = (steps[:, None] < steps[None, :]).astype(bf16)
    partial = jnp.zeros((groups, wide, model_width), f32)
    for e in range(experts_here):
        matches = named == (me * experts_here + e).astype(bf16)
        hit = jnp.any(matches, axis=0)
        gate = jnp.sum(jnp.where(matches, scale.astype(f32), 0.0), axis=0)
        slot = jnp.dot(hit.astype(bf16), earlier, preferred_element_type=f32).astype(jnp.int32)
        slot = jnp.where(hit, slot, -1)
        chosen = slot[:, None, :] == jnp.arange(slots, dtype=jnp.int32)[None, :, None]
        placing = chosen.astype(bf16)
        mixing = jnp.where(chosen, gate[:, None, :], 0.0).astype(bf16)
        picked = jnp.einsum("gct,gtd->gcd", placing, rows_all, preferred_element_type=f32)
        picked = picked.astype(bf16).reshape(groups * slots, model_width)
        gate_h = jnp.dot(picked, w_gate[e], preferred_element_type=f32)
        up_h = jnp.dot(picked, w_up[e], preferred_element_type=f32)
        act = (jax.nn.silu(gate_h) * up_h).astype(bf16)
        produced = jnp.dot(act, w_down[e], preferred_element_type=f32).astype(bf16)
        partial = partial + jnp.einsum(
            "gct,gcd->gtd",
            mixing,
            produced.reshape(groups, slots, model_width),
            preferred_element_type=f32,
        )
    partial = partial.astype(bf16).reshape(n, row_count, model_width)
    routed = ring_reduce(partial, n, 2)
    layer_out = (residual + routed).astype(bf16).reshape(seq_count, local_len, model_width)
    return jnp.transpose(layer_out, (1, 0, 2))[None]


def solution(mesh):
    return jax.shard_map(
        shards,
        mesh=mesh,
        in_specs=(
            P("dp", "expert", None, None),
            P("dp", "expert", None, None),
            P("dp", "expert", None, None),
            P("dp", None, None, None),
            P("dp", None),
            P("dp", "expert", None, None),
            P("dp", "expert", None, None),
            P(),
            P("dp", None, None),
            P("dp", None),
            P("expert", None, None),
            P("expert", None, None),
            P("expert", None, None),
        ),
        out_specs=P("dp", "expert", None, None),
        check_vma=False,
    )
```

```python
import functools

import jax
import jax.numpy as jnp
from jax import lax
from jax.experimental import pallas as pl
from jax.experimental.pallas import tpu as pltpu
from jax.sharding import PartitionSpec as P

score_scale = 192.0 ** (-0.5)
norm_eps = 1e-06
MESH = pl.DeviceIdType.MESH


def ring_place(n):
    chips = n // 2
    depth = chips // 2
    me = lax.axis_index("expert")
    core = me % 2
    chip = me // 2
    row, col = chip // 2, chip % 2
    pos = col * row + (1 - col) * (chips - 1 - row)

    def device(offset, core_of):
        p = (pos + offset + chips) % chips
        q = p // depth
        r = (1 - q) * p + q * (chips - 1 - p)
        return (2 * r + 1 - q) * 2 + core_of

    return me, core, device


def greet(targets):
    barrier = pltpu.get_barrier_semaphore()
    for target in targets:
        pl.semaphore_signal(barrier, inc=1, device_id={"expert": target}, device_id_type=MESH)
    pl.semaphore_wait(barrier, len(targets))


def remote(src, dst, send_sem, recv_sem, target):
    return pltpu.make_async_remote_copy(
        src_ref=src,
        dst_ref=dst,
        send_sem=send_sem,
        recv_sem=recv_sem,
        device_id={"expert": target},
        device_id_type=MESH,
    )


def gather_kernel(n, cut, x_ref, out_ref, ring_send, ring_recv, pair_send, pair_recv, own_sem):
    chips = n // 2
    half_ring = chips // 2
    rows = x_ref.shape[0]
    last = chips - 2
    me, core, device = ring_place(n)
    partner = device(0, 1 - core)
    ahead = (device(1, core), device(-1, core))
    spans = (pl.ds(0, cut), pl.ds(cut, rows - cut))
    greet((ahead[0], ahead[1], partner))

    def arrival(way, j):
        dist, half = (half_ring, way) if j == last else (j // 2 + 1, j % 2)
        return device(-dist if way == 0 else dist, core), spans[half]

    waits = []
    for way in (0, 1):
        for j in (0, 1):
            if j > last:
                continue
            if j == last and half_ring == 1:
                span = spans[way]
            else:
                span = spans[j]
            copy = remote(
                x_ref.at[span], out_ref.at[me, span],
                ring_send.at[way, j], ring_recv.at[way, j], ahead[way],
            )
            copy.start()
            waits.append(copy)
    share = remote(x_ref, out_ref.at[me], pair_send.at[2 * last + 2], pair_recv.at[2 * last + 2], partner)
    share.start()
    waits.append(share)
    keep = pltpu.make_async_copy(x_ref, out_ref.at[me], own_sem)
    keep.start()

    for j in range(last + 1):
        for way in (0, 1):
            slot, span = arrival(way, j)
            piece = out_ref.at[slot, span]
            remote(piece, piece, ring_send.at[way, j], ring_recv.at[way, j], ahead[way]).wait_recv()
            onward = j + 2
            if j >= last - 2 and j < last:
                onward = last if j == last - 2 + way else None
            if j == last:
                onward = None
            if onward is not None:
                copy = remote(piece, piece, ring_send.at[way, onward], ring_recv.at[way, onward], ahead[way])
                copy.start()
                waits.append(copy)
            index = 2 * j + way
            copy = remote(piece, piece, pair_send.at[index], pair_recv.at[index], partner)
            copy.start()
            waits.append(copy)

    for j in range(last + 1):
        for way in (0, 1):
            dist, half = (half_ring, way) if j == last else (j // 2 + 1, j % 2)
            slot = device(-dist if way == 0 else dist, 1 - core)
            piece = out_ref.at[slot, spans[half]]
            index = 2 * j + way
            remote(piece, piece, pair_send.at[index], pair_recv.at[index], partner).wait_recv()
    other = out_ref.at[partner]
    remote(other, other, pair_send.at[2 * last + 2], pair_recv.at[2 * last + 2], partner).wait_recv()
    for copy in waits:
        copy.wait_send()
    keep.wait()


def ring_gather(x, n, cut, collective_id):
    rows, cols = x.shape
    steps = n // 2 - 1
    return pl.pallas_call(
        functools.partial(gather_kernel, n, cut),
        out_shape=jax.ShapeDtypeStruct((n, rows, cols), x.dtype),
        in_specs=[pl.BlockSpec(memory_space=pltpu.VMEM)],
        out_specs=pl.BlockSpec(memory_space=pl.ANY),
        scratch_shapes=[
            pltpu.SemaphoreType.DMA((2, steps)),
            pltpu.SemaphoreType.DMA((2, steps)),
            pltpu.SemaphoreType.DMA((2 * steps + 1,)),
            pltpu.SemaphoreType.DMA((2 * steps + 1,)),
            pltpu.SemaphoreType.DMA,
        ],
        compiler_params=pltpu.CompilerParams(collective_id=collective_id, has_side_effects=True),
        cost_estimate=pl.CostEstimate(flops=0, bytes_accessed=16 * n * rows * cols, transcendentals=0),
        name="ring_gather_%d" % collective_id,
    )(x)


def reduce_kernel(
    n, rows_ref, mix_ref, out_ref, mine, paired, give, arrived, ring_send, ring_recv, pair_send, pair_recv
):
    chips = n // 2
    half_ring = chips // 2
    half = mine.shape[1] // 2
    last = chips - 2
    me, core, device = ring_place(n)
    partner = device(0, 1 - core)
    ahead = (device(1, core), device(-1, core))
    greet((ahead[0], ahead[1], partner))

    order = [half_ring]
    for k in range(half_ring - 1, 0, -1):
        order += [k, chips - k]
    order.append(0)
    depth = give.shape[0]
    shares, made, seen = {}, [], set()

    def weigh(k, core_of):
        dest = device(k, core_of)
        return jnp.dot(
            mix_ref[dest], rows_ref[dest // 2], preferred_element_type=jnp.float32
        ).astype(mine.dtype)

    def make():
        k = order[len(made)]
        slot = len(made) % depth
        if len(made) >= depth:
            shares[order[len(made) - depth]].wait_send()
        give[slot] = weigh(k, 1 - core)
        shares[k] = remote(give.at[slot], paired.at[k], pair_send.at[k], pair_recv.at[k], partner)
        shares[k].start()
        mine[k] = weigh(k, core)
        made.append(k)

    def bring(k):
        while k not in made or (len(made) < chips and len(made) < order.index(k) + 3):
            make()
        if k not in seen:
            seen.add(k)
            shares[k].wait_recv()

    def index_of(dist, h):
        return 0 if dist == half_ring else 1 + 2 * (half_ring - 1 - dist) + h

    def await_ring(way, j):
        piece = arrived.at[way, j]
        remote(piece, piece, ring_send.at[way, j], ring_recv.at[way, j], ahead[way]).wait_recv()

    sends = []
    for dist in range(half_ring, 0, -1):
        for turn in (0, 1):
            for way in (0, 1):
                if dist == half_ring:
                    if turn == 1:
                        continue
                    h = way
                elif dist == half_ring - 1:
                    h = 1 - way if turn == 0 else way
                else:
                    h = turn
                k = dist if way == 0 else chips - dist
                bring(k)
                span = pl.ds(h * half, half)
                total = mine[k, span].astype(jnp.float32) + paired[k, span].astype(jnp.float32)
                has_prior = dist < half_ring - 1 or (dist == half_ring - 1 and h == way)
                if has_prior:
                    j = index_of(dist + 1, h)
                    await_ring(way, j)
                    total = total + arrived[way, j].astype(jnp.float32)
                mine[k, span] = total.astype(mine.dtype)
                j = index_of(dist, h)
                copy = remote(
                    mine.at[k, span], arrived.at[way, j],
                    ring_send.at[way, j], ring_recv.at[way, j], ahead[way],
                )
                copy.start()
                sends.append(copy)
    bring(0)
    for h in (0, 1):
        span = pl.ds(h * half, half)
        total = mine[0, span].astype(jnp.float32) + paired[0, span].astype(jnp.float32)
        for way in (0, 1):
            j = index_of(1, h)
            await_ring(way, j)
            total = total + arrived[way, j].astype(jnp.float32)
        out_ref[span] = total
    for copy in sends:
        copy.wait_send()
    for k in order[chips - min(depth, chips) :]:
        shares[k].wait_send()


def ring_reduce(rows_in, mix, n, collective_id):
    rows = mix.shape[1]
    cols = rows_in.shape[2]
    chips = n // 2
    dtype = rows_in.dtype
    return pl.pallas_call(
        functools.partial(reduce_kernel, n),
        out_shape=jax.ShapeDtypeStruct((rows, cols), jnp.float32),
        in_specs=[pl.BlockSpec(memory_space=pltpu.VMEM)] * 2,
        out_specs=pl.BlockSpec(memory_space=pltpu.VMEM),
        scratch_shapes=[
            pltpu.VMEM((chips, rows, cols), dtype),
            pltpu.VMEM((chips, rows, cols), dtype),
            pltpu.VMEM((min(4, chips), rows, cols), dtype),
            pltpu.VMEM((2, chips - 1, rows // 2, cols), dtype),
            pltpu.SemaphoreType.DMA((2, chips - 1)),
            pltpu.SemaphoreType.DMA((2, chips - 1)),
            pltpu.SemaphoreType.DMA((chips,)),
            pltpu.SemaphoreType.DMA((chips,)),
        ],
        compiler_params=pltpu.CompilerParams(
            collective_id=collective_id, has_side_effects=True, vmem_limit_bytes=62 * 1024 * 1024
        ),
        cost_estimate=pl.CostEstimate(
            flops=2 * mix.size * cols, bytes_accessed=16 * n * rows * cols, transcendentals=0
        ),
        name="ring_reduce_%d" % collective_id,
    )(rows_in, mix)


def shards(
    hidden,
    queries,
    latents,
    mem_latents,
    lengths,
    ids,
    gates,
    norm_gain,
    w_uv,
    w_out,
    w_gate,
    w_up,
    w_down,
):
    f32, bf16 = jnp.float32, jnp.bfloat16
    local_len, seq_count, model_width = hidden.shape[1:]
    latent_dim = latents.shape[3]
    head_count = queries.shape[3] // latent_dim
    row_count = local_len * seq_count
    n = lax.axis_size("expert")
    dp_size = lax.axis_size("dp")
    me = lax.axis_index("expert")
    core = me % 2
    own_dp = lax.axis_index("dp")
    heads_here, _, value_dim = w_uv.shape
    top_count = ids.shape[3]

    half_heads = heads_here // 2
    uv_half = lax.dynamic_slice_in_dim(w_uv, core * half_heads, half_heads, 0)
    out_half = lax.dynamic_slice_in_dim(
        w_out, core * half_heads * value_dim, half_heads * value_dim, 0
    )
    uv_groups, out_groups, starts = [w_uv], [w_out], [own_dp * heads_here]
    swap = [(i, i ^ 1) for i in range(n)]
    sizes = [heads_here]
    for shift in range(1, dp_size):
        turn = [(i, (i + shift) % dp_size) for i in range(dp_size)]
        source = (own_dp - shift + dp_size) % dp_size
        uv_far = lax.ppermute(uv_half, "dp", turn)
        out_far = lax.ppermute(out_half, "dp", turn)
        uv_near = lax.ppermute(uv_far, "expert", swap)
        out_near = lax.ppermute(out_far, "expert", swap)
        uv_groups += [uv_far, uv_near]
        out_groups += [out_far, out_near]
        starts += [
            source * heads_here + core * half_heads,
            source * heads_here + (1 - core) * half_heads,
        ]
        sizes += [half_heads, half_heads]

    latent_rows = jnp.transpose(latents[0], (1, 0, 2)).reshape(row_count, latent_dim)
    ids_t = jnp.transpose(ids[0], (2, 1, 0)).reshape(top_count, row_count).astype(bf16)
    gates_t = jnp.transpose(gates[0], (2, 1, 0)).reshape(top_count, row_count)
    table = jnp.concatenate([ids_t, gates_t], axis=0).reshape(-1)
    table_rows = -(-table.shape[0] // (16 * latent_dim)) * 16
    table = jnp.pad(table, (0, table_rows * latent_dim - table.shape[0]))
    packed = jnp.concatenate([latent_rows, table.reshape(table_rows, latent_dim)], axis=0)
    all_rows = row_count + table_rows
    cut = (all_rows // 2 + 15) // 16 * 16
    gathered = ring_gather(packed, n, cut, 0)

    segment = gathered[:, :row_count].reshape(n, seq_count, local_len, latent_dim)
    segment = jnp.transpose(segment, (1, 0, 2, 3)).reshape(seq_count, n * local_len, latent_dim)
    memory = jnp.transpose(mem_latents[0], (1, 0, 2))
    mem_count = memory.shape[1]
    keys = jnp.concatenate([memory, segment], axis=1)
    query_rows = jnp.transpose(
        queries[0].reshape(local_len, seq_count, head_count, latent_dim), (1, 2, 0, 3)
    ).reshape(seq_count, head_count * local_len, latent_dim)
    scores = jnp.einsum("sql,sjl->sqj", query_rows, keys, preferred_element_type=f32) * score_scale
    key_pos = lax.broadcasted_iota(jnp.int32, scores.shape, 2) - mem_count
    own_pos = me * local_len + lax.broadcasted_iota(jnp.int32, scores.shape, 1) % local_len
    visible = (key_pos <= own_pos) & (key_pos < lengths[0][:, None, None])
    scores = jnp.where(visible | (key_pos < 0), scores, -jnp.inf)
    weights = jnp.exp(scores - jnp.max(scores, axis=2, keepdims=True))
    total = jnp.sum(weights, axis=2, keepdims=True)
    attended = jnp.einsum("sqj,sjl->sql", weights.astype(bf16), keys, preferred_element_type=f32)
    attended = (attended / total).astype(bf16)
    attended = attended.reshape(seq_count, head_count, local_len, latent_dim)

    attn_out = jnp.zeros((row_count, model_width), f32)
    for uv, out, start, size in zip(uv_groups, out_groups, starts, sizes):
        heads = lax.dynamic_slice_in_dim(attended, start, size, 1)
        values = jnp.einsum("shtl,hlv->sthv", heads, uv, preferred_element_type=f32).astype(bf16)
        attn_out = attn_out + jnp.dot(
            values.reshape(row_count, size * value_dim), out, preferred_element_type=f32
        )

    hidden_rows = jnp.transpose(hidden[0], (1, 0, 2)).reshape(row_count, model_width)
    residual = lax.optimization_barrier(hidden_rows).astype(f32) + attn_out
    mean_square = jnp.mean(residual * residual, axis=-1, keepdims=True)
    normed = (residual * lax.rsqrt(mean_square + norm_eps) * norm_gain.astype(f32)).astype(bf16)

    rows_all = ring_gather(normed, n, row_count // 2, 1)
    experts_here = w_gate.shape[0]
    expert_count = n * experts_here
    capacity = min(row_count, row_count * top_count // expert_count + 2)
    groups = n // 2
    wide = 2 * row_count
    slots = -(-2 * capacity // 16) * 16
    tables = gathered[:, row_count:].reshape(n, -1)[:, : 2 * top_count * row_count]
    tables = tables.reshape(groups, 2, 2, top_count, row_count)
    named = jnp.transpose(tables[:, :, 0], (2, 0, 1, 3)).reshape(top_count, groups, wide)
    scale = jnp.transpose(tables[:, :, 1], (2, 0, 1, 3)).reshape(top_count, groups, wide)
    rows_all = rows_all.reshape(groups, wide, model_width)
    steps = jnp.arange(wide, dtype=jnp.int32)
    earlier = (steps[:, None] < steps[None, :]).astype(bf16)
    made_rows, mixes = [], []
    for e in range(experts_here):
        matches = named == (me * experts_here + e).astype(bf16)
        hit = jnp.any(matches, axis=0)
        gate = jnp.sum(jnp.where(matches, scale.astype(f32), 0.0), axis=0)
        slot = jnp.dot(hit.astype(bf16), earlier, preferred_element_type=f32).astype(jnp.int32)
        slot = jnp.where(hit, slot, -1)
        chosen = slot[:, None, :] == jnp.arange(slots, dtype=jnp.int32)[None, :, None]
        placing = chosen.astype(bf16)
        slot_t = jnp.where(hit, slot, -1).reshape(n, row_count)
        chosen_t = slot_t[:, :, None] == jnp.arange(slots, dtype=jnp.int32)[None, None, :]
        mixes.append(jnp.where(chosen_t, gate.reshape(n, row_count)[:, :, None], 0.0).astype(bf16))
        picked = jnp.einsum("gct,gtd->gcd", placing, rows_all, preferred_element_type=f32)
        picked = picked.astype(bf16).reshape(groups * slots, model_width)
        gate_h = jnp.dot(picked, w_gate[e], preferred_element_type=f32)
        up_h = jnp.dot(picked, w_up[e], preferred_element_type=f32)
        act = (jax.nn.silu(gate_h) * up_h).astype(bf16)
        produced = jnp.dot(act, w_down[e], preferred_element_type=f32).astype(bf16)
        made_rows.append(produced.reshape(groups, slots, model_width))
    made_rows = made_rows[0] if experts_here == 1 else jnp.concatenate(made_rows, axis=1)
    mixing = mixes[0] if experts_here == 1 else jnp.concatenate(mixes, axis=2)
    routed = ring_reduce(made_rows, mixing, n, 2)
    layer_out = (residual + routed).astype(bf16).reshape(seq_count, local_len, model_width)
    return jnp.transpose(layer_out, (1, 0, 2))[None]


def solution(mesh):
    return jax.shard_map(
        shards,
        mesh=mesh,
        in_specs=(
            P("dp", "expert", None, None),
            P("dp", "expert", None, None),
            P("dp", "expert", None, None),
            P("dp", None, None, None),
            P("dp", None),
            P("dp", "expert", None, None),
            P("dp", "expert", None, None),
            P(),
            P("dp", None, None),
            P("dp", None),
            P("expert", None, None),
            P("expert", None, None),
            P("expert", None, None),
        ),
        out_specs=P("dp", "expert", None, None),
        check_vma=False,
    )
```
